32 devices in a mesh: days: 4 (over y, x), space: 8 (over z, core).
Axes of the slice: x: 2, y: 2, z: 4, core: 2. Of those that a mesh axis runs over, the one named last changes fastest.
Arguments:
- fields: bfloat16 [640, 32, 1440], P('days', 'space')
- month_label: int32 [640], P('days'), may hold values from 0 to 11, as said below
- row_index: int32 [32], P('space'), may hold values from 0 to 31
- area_table: float32 [32], replicated, may hold values from 0.05 to 1
- basis: bfloat16 [64, 32, 1440], P(None, 'space'), may hold values from -6 to 6
Outputs:
- eofs: float32 [64, 32, 1440], P(None, 'space')
- pcs: float32 [640, 64], P('days')
The draws below stay inside these ranges and needn't reach their ends.
Inputs may be any that keep to these rules, and one draw needn't show every extreme that they name: `month_label`: each day's label differs from floor(12 * day / 640) by at most one; the first day with a given value of floor(12 * day / 640) carries exactly that value; every month labels at least one day.
All inputs are finite; a program needn't handle non-finite values.
Results may differ from the reference program's by a relative error of at most 0.0003.
Values sent between devices are 32-bit elements; how exact they have to be, the bound alone decides.
A program may use at most 64 MiB of HBM per device.

```python
import math
import jax
import jax.numpy as jnp
from jax import lax

LON = 1440
MODES = 64
ITERS = 2
LAT_DEV = 4
LAT = 32
DAYS = 640
N_SPACE = 8


def month_series(key):
    day = jnp.arange(DAYS, dtype=jnp.int32)
    base = day * 12 // DAYS
    first = base != (day - 1) * 12 // DAYS
    jitter = jax.random.randint(jax.random.fold_in(key, 7), (DAYS,), -1, 2)
    return jnp.where(first, base, jnp.clip(base + jitter, 0, 11)).astype(jnp.int32)


def draw_month_label(key, part):
    return month_series(key)


def draw_fields(key, part):
    labels = month_series(key)
    season = jax.random.normal(jax.random.fold_in(key, 11), (12, LAT, LON), jnp.float32)
    noise = jax.random.normal(jax.random.fold_in(key, 13), (DAYS, LAT, LON), jnp.float32)
    values = 2.0 * season[labels] + noise
    return values.astype(jnp.bfloat16)


def touch_ends(entries, rng, low, top_value):
    dims = entries.shape
    place = [jax.random.randint(jax.random.fold_in(rng, axis), (), 0, dims[axis]) for axis in range(len(dims))]
    entries = entries.at[tuple(place)].set(low)
    longest = dims.index(max(dims))
    place[longest] = (place[longest] + 1) % dims[longest]
    return entries.at[tuple(place)].set(top_value)


def block_scale(rng, extent, shards, smallest, top_value):
    gain, own = 1.0, jax.random.fold_in(rng, 6)
    for dim, shards_of in shards:
        steps = jnp.exp(jax.random.uniform(jax.random.fold_in(own, dim), (shards_of,), jnp.float32, smallest / len(shards), top_value / len(shards)))
        gain = gain * jnp.repeat(steps, extent[dim] // shards_of).reshape([-1 if axis == dim else 1 for axis in range(len(extent))])
    return gain


def scatter_about(own_key, dims, deviation, bound, cuts=(), kind=jnp.bfloat16):
    values = jax.random.normal(own_key, dims, jnp.float32) * deviation
    if len(cuts) > 0:
        values = block_scale(own_key, dims, cuts, -0.22, 0.18) * values
    return jnp.clip(values, min=-bound, max=bound).astype(kind)


def setup_inputs(seed: int = 0) -> dict:
    seeds = jax.random.split(jax.random.key(seed), 6)
    fields = draw_fields(jax.random.fold_in(seeds[5], 71), 0)
    month_label = draw_month_label(jax.random.fold_in(seeds[5], 71), 0)
    row_index = touch_ends(jax.random.randint(seeds[2], (LAT,), 0, LAT), jax.random.fold_in(seeds[2], 1), 0, LAT - 1).astype(jnp.int32)
    area_table = jnp.clip(jnp.exp(jax.random.uniform(seeds[3], (LAT,), jnp.float32, math.log(0.05), math.log(1.0))), 0.05, 1.0)
    basis = scatter_about(seeds[4], (MODES, LAT, LON), 1.0, 6.0, ((1, 8),))
    return dict(fields=fields, month_label=month_label, row_index=row_index, area_table=area_table, basis=basis)


HIGH = lax.Precision.HIGHEST

def reference(fields, month_label, row_index, area_table, basis):
    months = jnp.arange(12, dtype=jnp.int32)
    onehot = (month_label[None, :] == months[:, None]).astype(jnp.float32)
    counts = lax.optimization_barrier(jnp.sum(onehot, axis=1))

    def block_fields(index):
        return lax.dynamic_slice_in_dim(fields, (index * LAT_DEV).astype(jnp.int32), LAT_DEV, 1).astype(jnp.float32)

    def add_sums(index):
        return jnp.einsum('md,dlc->mlc', onehot, block_fields(index), precision=HIGH)
    sums = lax.map(add_sums, jnp.arange(N_SPACE, dtype=jnp.int32))
    climate = sums / counts[None, :, None, None]
    scale = jnp.sqrt(area_table[row_index])

    def anomaly(index):
        seasonal = jnp.einsum('md,mlc->dlc', onehot, climate[index], precision=HIGH)
        rows = lax.dynamic_slice_in_dim(scale, (index * LAT_DEV).astype(jnp.int32), LAT_DEV, 0)
        return (block_fields(index) - seasonal) * rows[None, :, None]

    def project(patterns):

        def step(total, index):
            piece = lax.dynamic_slice_in_dim(patterns, (index * LAT_DEV).astype(jnp.int32), LAT_DEV, 1)
            return (total + jnp.einsum('dlc,klc->dk', anomaly(index), piece, precision=HIGH), None)
        start = jnp.zeros((DAYS, MODES), jnp.float32)
        total, _ = lax.scan(step, start, jnp.arange(N_SPACE, dtype=jnp.int32))
        return total
    pcs = project(basis.astype(jnp.float32))
    for step_count in range(ITERS):

        def cover_block(index):
            return jnp.einsum('dk,dlc->klc', pcs, anomaly(index), precision=HIGH) / DAYS
        blocks = lax.map(cover_block, jnp.arange(N_SPACE, dtype=jnp.int32))
        cover = jnp.moveaxis(blocks, 0, 1).reshape(MODES, LAT * LON)
        gram = jnp.dot(cover, cover.T, precision=HIGH)
        lower = jnp.linalg.cholesky(gram)
        solved = lax.linalg.triangular_solve(lower, cover, left_side=True, lower=True)
        eofs = solved.reshape(MODES, LAT, LON)
        pcs = project(eofs)
    return (eofs, pcs)
```

```python
import functools

import jax
import jax.numpy as jnp
from jax import lax
from jax.experimental import pallas as pl
from jax.experimental.pallas import tpu as pltpu
from jax.sharding import PartitionSpec as P

ITERS = 2
MONTHS = 12
MESH = pl.DeviceIdType.MESH
HIGH = lax.Precision.HIGHEST
F32 = jnp.float32
BF16 = jnp.bfloat16
LANES = 128
CHUNK = 3 * LANES
EXTRA = 8
GRAM_AT = LANES // 2
BLOCK = 4


def nt(a, b, **kw):
    return lax.dot_general(a, b, (((1,), (1,)), ((), ())), preferred_element_type=F32, **kw)


def nn(a, b, **kw):
    return lax.dot_general(a, b, (((1,), (0,)), ((), ())), preferred_element_type=F32, **kw)


def split3(x):
    high = x.astype(BF16)
    rest = x - high.astype(F32)
    mid = rest.astype(BF16)
    low = (rest - mid.astype(F32)).astype(BF16)
    return jnp.concatenate([high, mid, low], axis=0)


def join3(x, n):
    return x[:n] + (x[n : 2 * n] + x[2 * n :])


def tree(terms):
    while len(terms) > 1:
        terms = [terms[i] + terms[i + 1] for i in range(0, len(terms), 2)]
    return terms[0]


def inverse_factor(tile):
    n = tile.shape[0]
    lane = lax.broadcasted_iota(jnp.int32, tile.shape, 1)
    sub = lax.broadcasted_iota(jnp.int32, tile.shape, 0)
    work = jnp.where(lane < GRAM_AT, (lane == sub).astype(F32), tile)
    for start in range(0, n, BLOCK):
        top = start // 8 * 8
        part = work[top:]
        rows = lax.broadcasted_iota(jnp.int32, part.shape, 0) + top
        at = GRAM_AT + start
        columns = [jnp.broadcast_to(part[:, at + t : at + t + 1], part.shape) for t in range(BLOCK)]
        for t in range(BLOCK):
            j = start + t
            k = j - top
            inv = lax.rsqrt(columns[t][k : k + 1])
            row = part[k : k + 1] * inv
            column = jnp.where(rows > j, columns[t] * inv, 0.0)
            for u in range(t + 1, BLOCK):
                columns[u] = columns[u] - column * column[k + u - t : k + u - t + 1]
            part = jnp.where(rows == j, row, part - column * row)
        work = part if top == 0 else jnp.concatenate([work[:top], part], axis=0)
    return work[:, :n]


def kernel(nd, ns, f_hbm, b_hbm, i_ref, a_ref, l_ref, eofs_ref, pcs_ref,
           f_in, b_in, own_f, send_f, recv_f, part_f, s_ref,
           u_out, r_one, v_out, r_two, blk, tl, c_send, c_recv, c_all,
           sem_l, sem_f, sem_one, sem_two, sem_b, sem_fw, sem_c, sem_g):
    dl, lat, lon = f_in.shape
    modes = eofs_ref.shape[0]
    hm = modes // 2
    base = dl // LANES * LANES
    tail = dl - base
    width = base + LANES
    nz = ns // 2
    chunks = [(at, min(CHUNK, lon - at)) for at in range(0, lon, CHUNK)]
    n_days = nd * dl
    day, space = lax.axis_index("days"), lax.axis_index("space")
    x, y = lax.rem(day, 2), lax.div(day, 2)
    c, z = lax.rem(space, 2), lax.div(space, 2)
    to_x, to_y, to_d = day + 1 - 2 * x, day + 2 - 4 * y, nd - 1 - day
    other = space + 1 - 2 * c
    row_of = (x, lat // 2 + y)
    row_out = (1 - x, lat // 2 + 1 - y)

    def flip(v, k):
        for bit in range(k.bit_length()):
            if (k >> bit) & 1:
                v = v + (1 << bit) * (1 - 2 * lax.rem(lax.div(v, 1 << bit), 2))
        return v

    def z_peer(k):
        return flip(z, k) * 2 + c

    started = []

    def describe(src, dst, sems, index, device):
        return pltpu.make_async_remote_copy(
            src_ref=src, dst_ref=dst, send_sem=sems.at[(0,) + index], recv_sem=sems.at[(1,) + index],
            device_id=device, device_id_type=MESH)

    def put(src, dst, sems, index, device):
        d = describe(src, dst, sems, index, device)
        d.start()
        started.append(d)

    def got(dst, sems, index, device):
        describe(dst, dst, sems, index, device).wait_recv()

    core = {"space": other}
    barrier = pltpu.get_barrier_semaphore()
    friends = [core] + [{"space": z_peer(k)} for k in range(1, nz)]
    for d in (to_x, to_y, to_d):
        friends += [{"days": d}, {"days": d, "space": other}]
    for friend in friends:
        pl.semaphore_signal(barrier, inc=1, device_id=friend, device_id_type=MESH)
    load_f = pltpu.make_async_copy(f_hbm, f_in, sem_l.at[0])
    load_b = pltpu.make_async_copy(b_hbm, b_in, sem_l.at[1])
    load_f.start()
    load_b.start()
    for l in range(lat):
        s_ref[l] = jnp.sqrt(jnp.full((1, 1), a_ref[i_ref[l]], F32))
    load_f.wait()
    for l in range(lat):
        own_f[l] = f_in[:, l, :]

    def fill(ab, i):
        at, w = chunks[i]
        send_f[ab, i, :, :w] = own_f[row_out[ab], :, at : at + w].astype(F32)

    def send_fields(i):
        w = chunks[i][1]
        for ab, to in ((0, to_x), (1, to_y)):
            put(send_f.at[ab, i], recv_f.at[ab, i], sem_f, (ab, i), {"days": to})

    early = len(chunks) - 1
    for i in range(len(chunks)):
        for ab in range(2):
            fill(ab, i)
        if i == 0:
            pl.semaphore_wait(barrier, len(friends))
        if i < early:
            send_fields(i)

    load_b.wait()
    total = None
    for l in range(lat):
        term = nt(b_in[:, l, :], own_f[l]) * s_ref[l]
        total = term if total is None else total + term

    lane = lax.broadcasted_iota(jnp.int32, (1, LANES), 1)

    def hot_of(labels):
        rows = lax.broadcasted_iota(jnp.int32, (LANES, dl), 0) - tail
        return (rows.astype(F32) == labels).astype(F32).astype(BF16)

    def reduce(st, hot):
        rows = hm + EXTRA if st == 0 else hm
        put(u_out.at[st, 0, 1 - c], r_one.at[st, 0], sem_one, (st, 0), core)
        if st > 0:
            for p, to in ((0, to_x), (1, to_y)):
                put(u_out.at[st, 1 + p, c], r_one.at[st, 1 + 2 * p], sem_one, (st, 1 + 2 * p), {"days": to})
                put(u_out.at[st, 1 + p, 1 - c], r_one.at[st, 2 + 2 * p], sem_one, (st, 2 + 2 * p), {"days": to, "space": other})
        return rows

    def finish(st, hot, last):
        rows = hm + EXTRA if st == 0 else hm
        mine = u_out[st, 0, c]
        got(r_one.at[st, 0], sem_one, (st, 0), core)
        near = r_one[st, 0]
        value = mine[:, :width] + near[:, :width]
        if st > 0:
            gram = (mine[:, base:width] + near[:, base:width], mine[:, width:] + near[:, width:])
            parts = []
            for p, to in ((0, to_x), (1, to_y)):
                got(r_one.at[st, 1 + 2 * p], sem_one, (st, 1 + 2 * p), {"days": to})
                got(r_one.at[st, 2 + 2 * p], sem_one, (st, 2 + 2 * p), {"days": to, "space": other})
                far = r_one[st, 1 + 2 * p, :, :width] + r_one[st, 2 + 2 * p, :, :width]
                value = value + far
                parts.append(gram[p] + far[:, base:])
            low = jnp.where(lane < GRAM_AT, value[:, base:], parts[0] + parts[1])
            v_out[st, :, :base] = value[:, :base]
            v_out[st, :, base:] = low
        else:
            v_out[st] = value
        for k in range(1, nz):
            put(v_out.at[st], r_two.at[st, k - 1], sem_two, (st, k - 1), {"space": z_peer(k)})
        for k in range(1, nz):
            got(r_two.at[st, k - 1], sem_two, (st, k - 1), {"space": z_peer(k)})
        value = tree([v_out[st]] + [r_two[st, k - 1] for k in range(1, nz)])
        month = join3(nt(split3(value[:, :dl]), hot), hm)
        blk[st, 0, c, :hm, :base] = value[:, :base]
        blk[st, 0, c, :hm, base:] = value[:, base:] + month
        if st == 0:
            names = jnp.broadcast_to(l_ref[...].astype(F32), (EXTRA, dl))
            blk[st, 0, c, hm:, :base] = names[:, :base]
            blk[st, 0, c, hm:, base:] = nt(jnp.ones((EXTRA, dl), BF16), hot)
            blk[st, 0, c, hm:, base:dl] = names[:, base:]
        mine = blk.at[st, 0, c, pl.ds(0, rows)]
        put(mine, mine, sem_b, (st, 3), core)
        for p, to in ((0, to_x), (1, to_y), (2, to_d)):
            if p < 2 and not last:
                put(mine, blk.at[st, 1 + p, c, pl.ds(0, rows)], sem_b, (st, p), {"days": to})
            else:
                put(blk.at[st, 0, c, pl.ds(0, rows), pl.ds(base, LANES)], tl.at[st, p, c, pl.ds(0, rows)], sem_b, (st, p), {"days": to})
        theirs = blk.at[st, 0, 1 - c, pl.ds(0, rows)]
        got(theirs, sem_b, (st, 3), core)

    def landed(st, last, p, half):
        rows = hm + EXTRA if st == 0 else hm
        if p < 2 and not last:
            return blk.at[st, 1 + p, half, pl.ds(0, rows)]
        return tl.at[st, p, half, pl.ds(0, rows)]

    def forward(st, last):
        for p, to in ((0, to_x), (1, to_y), (2, to_d)):
            ref = landed(st, last, p, c)
            got(ref, sem_b, (st, p), {"days": to})
            put(ref, ref, sem_fw, (st, p), core)
        for p in range(3):
            got(landed(st, last, p, 1 - c), sem_fw, (st, p), core)

    def both(st, b):
        return jnp.concatenate([blk[st, b, 0, :hm], blk[st, b, 1, :hm]], axis=0)

    def tiles(st, last):
        out = [both(st, 0)[:, base:]]
        for p in range(3):
            if p < 2 and not last:
                out.append(both(st, 1 + p)[:, base:])
            else:
                out.append(jnp.concatenate([tl[st, p, 0, :hm], tl[st, p, 1, :hm]], axis=0))
        return out

    def mean_of(st, last, scale):
        sums = tree(tiles(st, last))
        inside = (lane >= tail) & (lane < tail + MONTHS)
        return split3(jnp.where(inside, sums * scale, 0.0))

    def center(value, mean, hot):
        return value - join3(nn(mean, hot), modes)

    own_hot = hot_of(l_ref[...].astype(F32))
    for half in range(2):
        u_out[0, 0, half] = jnp.zeros((hm, width + LANES), F32)
        u_out[0, 0, half, :, :dl] = total[half * hm : (half + 1) * hm]
    reduce(0, own_hot)
    finish(0, own_hot, False)
    for i in range(early, len(chunks)):
        send_fields(i)
    forward(0, False)
    hots = [own_hot] + [hot_of(blk[0, 1 + p, 0, hm : hm + 1, :dl]) for p in range(2)]
    counts = tree([blk[0, b, 0, hm : hm + 1, base:] for b in range(3)] + [tl[0, 2, 0, hm : hm + 1]])
    per_day = 1.0 / jnp.maximum(counts, 1.0)
    mean = mean_of(0, False, per_day)
    patterns = [split3(center(both(0, b)[:, :dl], mean, hots[b])) for b in range(3)]

    for it in range(ITERS):
        st = it + 1
        last = it == ITERS - 1
        for i, (at, w) in enumerate(chunks):
            for ab, to, back in ((0, to_x, to_y), (1, to_y, to_x)):
                if it == 0:
                    got(recv_f.at[ab, i], sem_f, (ab, i), {"days": to})
                    part_f[ab, :, at : at + w] = recv_f[ab, i, :, :w].astype(BF16)
                cover = join3(nn(patterns[0], own_f[row_of[ab], :, at : at + w])
                              + nn(patterns[1 + ab], part_f[ab, :, at : at + w]), modes)
                c_send[it, ab, i, :, :w] = cover
                put(c_send.at[it, ab, i], c_recv.at[it, ab, i], sem_c, (it, ab, i), {"days": back})
        raw = [None] * 3
        gram = [None] * 2

        def add(sums, k, term):
            sums[k] = term if sums[k] is None else sums[k] + term

        def spread(i):
            w = chunks[i][1]
            for ab, to in ((0, to_x), (1, to_y)):
                ref = c_all.at[row_of[ab], i]
                put(ref, ref, sem_g, (ab, i), {"days": to})

        for i, (at, w) in enumerate(chunks):
            for ab, back in ((0, to_y), (1, to_x)):
                got(c_recv.at[it, ab, i], sem_c, (it, ab, i), {"days": back})
                scale = s_ref[row_of[ab]]
                cover = (c_send[it, ab, i, :, :w] + c_recv[it, ab, i, :, :w]) * (scale * (1.0 / n_days))
                if last:
                    c_all[row_of[ab], i, :, :w] = cover
                padded = jnp.concatenate([jnp.zeros((GRAM_AT, w), F32), cover], axis=0)
                add(gram, ab, nt(cover, padded, precision=HIGH))
                cover3 = split3(cover * scale)
                add(raw, 0, nt(cover3, own_f[row_of[ab], :, at : at + w]))
                add(raw, 1 + ab, nt(cover3, part_f[ab, :, at : at + w]))
            if last and i == 0:
                spread(0)
        for b in range(3):
            full = join3(raw[b], modes)
            for half in range(2):
                cut = slice(half * hm, (half + 1) * hm)
                u_out[st, b, half, :, base:width] = gram[max(b - 1, 0)][cut]
                if b == 0:
                    u_out[st, b, half, :, width:] = gram[1][cut]
                else:
                    u_out[st, b, half, :, width:] = jnp.zeros((hm, LANES), F32)
                u_out[st, b, half, :, :dl] = full[cut]
        reduce(st, own_hot)
        if last:
            for i in range(1, len(chunks)):
                spread(i)
        finish(st, own_hot, last)
        inv = inverse_factor(both(st, 0)[:, base:])
        if not last:
            forward(st, last)
            mean = mean_of(st, last, per_day)
            patterns = [split3(nn(inv, center(both(st, b)[:, :dl], mean, hots[b]), precision=HIGH)) for b in range(3)]
        else:
            for i, (at, w) in enumerate(chunks):
                for ab, to in ((0, to_x), (1, to_y)):
                    got(c_all.at[row_out[ab], i], sem_g, (ab, i), {"days": to})
                for l in range(lat):
                    eofs_ref[:, l, at : at + w] = nn(inv, c_all[l, i, :, :w], precision=HIGH)
            forward(st, last)
            mean = mean_of(st, last, per_day)
            pcs_ref[...] = nn(inv, center(both(st, 0)[:, :dl], mean, own_hot), precision=HIGH)
    for d in started:
        d.wait_send()


def solution(mesh):
    nd, ns = mesh.shape["days"], mesh.shape["space"]

    def local(fields, month_label, row_index, area_table, basis):
        dl, lat, lon = fields.shape
        modes = basis.shape[0]
        hm, nz = modes // 2, ns // 2
        base = dl // LANES * LANES
        width = base + LANES
        if nd != 4 or lat != nd or modes > GRAM_AT or dl - base + MONTHS > GRAM_AT or nz & (nz - 1):
            raise ValueError("unsupported sizes")
        n = -(-lon // CHUNK)
        stages = ITERS + 1
        v, dma = pltpu.VMEM, pltpu.SemaphoreType.DMA
        eofs, pcs = pl.pallas_call(
            functools.partial(kernel, nd, ns),
            out_shape=(jax.ShapeDtypeStruct((modes, lat, lon), F32), jax.ShapeDtypeStruct((modes, dl), F32)),
            in_specs=[pl.BlockSpec(memory_space=pl.ANY)] * 2 + [pl.BlockSpec(memory_space=pltpu.SMEM)] * 2
            + [pl.BlockSpec(memory_space=v)],
            out_specs=(pl.BlockSpec(memory_space=v),) * 2,
            scratch_shapes=[
                v((dl, lat, lon), BF16),
                v((modes, lat, lon), BF16),
                v((lat, dl, lon), BF16),
                v((2, n, dl, CHUNK), F32),
                v((2, n, dl, CHUNK), F32),
                v((2, dl, lon), BF16),
                v((lat, 1, 1), F32),
                v((stages, 3, 2, hm, width + LANES), F32),
                v((stages, 5, hm, width + LANES), F32),
                v((stages, hm, width), F32),
                v((stages, nz - 1, hm, width), F32),
                v((stages, 3, 2, hm + EXTRA, width), F32),
                v((stages, 3, 2, hm + EXTRA, LANES), F32),
                v((ITERS, 2, n, modes, CHUNK), F32),
                v((ITERS, 2, n, modes, CHUNK), F32),
                v((lat, n, modes, CHUNK), F32),
                dma((2,)), dma((2, 2, n)), dma((2, stages, 5)), dma((2, stages, nz - 1)),
                dma((2, stages, 4)), dma((2, stages, 3)), dma((2, ITERS, 2, n)), dma((2, 2, n)),
            ],
            compiler_params=pltpu.CompilerParams(
                collective_id=0, has_side_effects=True, vmem_limit_bytes=60 * 1024 * 1024),
        )(fields, basis, row_index, area_table, month_label[None, :])
        return eofs, pcs.T

    placed = (P("days", "space", None), P("days"), P("space"), P(), P(None, "space", None))
    return jax.shard_map(
        local,
        mesh=mesh,
        in_specs=placed,
        out_specs=(P(None, "space", None), P("days", None)),
        check_vma=False,
    )
```

```python
import functools

import jax
import jax.numpy as jnp
from jax import lax
from jax.experimental import pallas as pl
from jax.experimental.pallas import tpu as pltpu
from jax.sharding import PartitionSpec as P

ITERS = 2
MONTHS = 12
MESH = pl.DeviceIdType.MESH
HIGH = lax.Precision.HIGHEST
F32 = jnp.float32
BF16 = jnp.bfloat16
LANES = 128
CHUNK = 3 * LANES
EXTRA = 8
GRAM_AT = LANES // 2
BLOCK = 4


def nt(a, b, **kw):
    return lax.dot_general(a, b, (((1,), (1,)), ((), ())), preferred_element_type=F32, **kw)


def nn(a, b, **kw):
    return lax.dot_general(a, b, (((1,), (0,)), ((), ())), preferred_element_type=F32, **kw)


def split3(x):
    high = x.astype(BF16)
    rest = x - high.astype(F32)
    mid = rest.astype(BF16)
    low = (rest - mid.astype(F32)).astype(BF16)
    return jnp.concatenate([high, mid, low], axis=0)


def join3(x, n):
    return x[:n] + (x[n : 2 * n] + x[2 * n :])


def tree(terms):
    while len(terms) > 1:
        terms = [terms[i] + terms[i + 1] for i in range(0, len(terms), 2)]
    return terms[0]


def pack(x, tail):
    rows = x.shape[0] * tail // LANES
    return jnp.concatenate([x[at : at + rows] for at in range(0, x.shape[0], rows)], axis=1)


def unpack(x, tail):
    return jnp.concatenate([x[:, at : at + tail] for at in range(0, LANES, tail)], axis=0)


def inverse_factor(tile):
    n = tile.shape[0]
    lane = lax.broadcasted_iota(jnp.int32, tile.shape, 1)
    sub = lax.broadcasted_iota(jnp.int32, tile.shape, 0)
    work = jnp.where(lane < GRAM_AT, (lane == sub).astype(F32), tile)
    for start in range(0, n, BLOCK):
        top = start // 8 * 8
        part = work[top:]
        rows = lax.broadcasted_iota(jnp.int32, part.shape, 0) + top
        at = GRAM_AT + start
        columns = [jnp.broadcast_to(part[:, at + t : at + t + 1], part.shape) for t in range(BLOCK)]
        for t in range(BLOCK):
            j = start + t
            k = j - top
            inv = lax.rsqrt(columns[t][k : k + 1])
            row = part[k : k + 1] * inv
            column = jnp.where(rows > j, columns[t] * inv, 0.0)
            for u in range(t + 1, BLOCK):
                columns[u] = columns[u] - column * column[k + u - t : k + u - t + 1]
            part = jnp.where(rows == j, row, part - column * row)
        work = part if top == 0 else jnp.concatenate([work[:top], part], axis=0)
    return work[:, :n]


def last_kernel(inv_ref, cover_ref, pcs_ref, eofs_ref, out_ref):
    inv = inv_ref[...]
    for l in range(eofs_ref.shape[1]):
        eofs_ref[:, l, :] = nn(inv, cover_ref[l, 0], precision=HIGH)
    out_ref[...] = pcs_ref[...]


def kernel(nd, ns, f_hbm, b_hbm, i_ref, a_ref, l_ref, cover_hbm, inv_ref, pcs_ref,
           f_in, b_in, own_f, send_f, recv_f, send_t, recv_t, part_f, s_ref,
           u_out, r_one, v_out, r_two, blk, tl, c_send, c_recv, c_all, t_send, t_recv, t_all,
           sem_l, sem_f, sem_one, sem_two, sem_b, sem_fw, sem_c, sem_g, sem_o):
    dl, lat, lon = f_in.shape
    modes = inv_ref.shape[0]
    hm = modes // 2
    base = dl // LANES * LANES
    tail = dl - base
    width = base + LANES
    nz = ns // 2
    chunks = [(at, min(CHUNK, lon - at)) for at in range(0, lon, CHUNK)]
    n_days = nd * dl
    rest = lon % LANES
    final = len(chunks) - 1
    full = [w // LANES * LANES for _, w in chunks]
    day, space = lax.axis_index("days"), lax.axis_index("space")
    x, y = lax.rem(day, 2), lax.div(day, 2)
    c, z = lax.rem(space, 2), lax.div(space, 2)
    to_x, to_y, to_d = day + 1 - 2 * x, day + 2 - 4 * y, nd - 1 - day
    other = space + 1 - 2 * c
    row_of = (x, lat // 2 + y)
    row_out = (1 - x, lat // 2 + 1 - y)

    def flip(v, k):
        for bit in range(k.bit_length()):
            if (k >> bit) & 1:
                v = v + (1 << bit) * (1 - 2 * lax.rem(lax.div(v, 1 << bit), 2))
        return v

    def z_peer(k):
        return flip(z, k) * 2 + c

    started = []

    def describe(src, dst, sems, index, device):
        return pltpu.make_async_remote_copy(
            src_ref=src, dst_ref=dst, send_sem=sems.at[(0,) + index], recv_sem=sems.at[(1,) + index],
            device_id=device, device_id_type=MESH)

    def put(src, dst, sems, index, device):
        d = describe(src, dst, sems, index, device)
        d.start()
        started.append(d)

    def got(dst, sems, index, device):
        describe(dst, dst, sems, index, device).wait_recv()

    core = {"space": other}
    barrier = pltpu.get_barrier_semaphore()
    friends = [core] + [{"space": z_peer(k)} for k in range(1, nz)]
    for d in (to_x, to_y, to_d):
        friends += [{"days": d}, {"days": d, "space": other}]
    for friend in friends:
        pl.semaphore_signal(barrier, inc=1, device_id=friend, device_id_type=MESH)
    load_f = pltpu.make_async_copy(f_hbm, f_in, sem_l.at[0])
    load_b = pltpu.make_async_copy(b_hbm, b_in, sem_l.at[1])
    load_f.start()
    load_b.start()
    for l in range(lat):
        s_ref[l] = jnp.sqrt(jnp.full((1, 1), a_ref[i_ref[l]], F32))
    load_f.wait()

    def move(act, src, dst, src_t, dst_t, i, sems, index, device):
        w = pl.ds(0, full[i])
        if full[i]:
            act(src.at[:, w], dst.at[:, w], sems, index + (i,), device)
        if i == final and rest:
            act(src_t, dst_t, sems, index + (i + 1,), device)

    def take(src, dst, sems, index, device):
        got(dst, sems, index, device)

    def value_of(ref, ref_t, i):
        main = ref[:, : full[i]]
        if i < final or not rest:
            return main
        return jnp.concatenate([main, unpack(ref_t[...], rest)], axis=1)

    def fill(ab, i):
        at, w = chunks[i]
        value = own_f[row_out[ab], :, at : at + w].astype(F32)
        send_f[ab, i, :, : full[i]] = value[:, : full[i]]
        if full[i] < w:
            send_t[ab] = pack(value[:, full[i] :], rest)

    def send_fields(i):
        for ab, to in ((0, to_x), (1, to_y)):
            move(put, send_f.at[ab, i], recv_f.at[ab, i], send_t.at[ab], recv_t.at[ab], i, sem_f, (ab,), {"days": to})

    early = len(chunks) - 1
    for i in range(len(chunks)):
        at, w = chunks[i]
        for l in range(lat):
            own_f[l, :, at : at + w] = f_in[:, l, at : at + w]
        for ab in range(2):
            fill(ab, i)
        if i == 0:
            pl.semaphore_wait(barrier, len(friends))
        if i < early:
            send_fields(i)

    load_b.wait()
    total = None
    for l in range(lat):
        term = nt(b_in[:, l, :], own_f[l]) * s_ref[l]
        total = term if total is None else total + term

    lane = lax.broadcasted_iota(jnp.int32, (1, LANES), 1)

    def hot_of(labels):
        rows = lax.broadcasted_iota(jnp.int32, (LANES, dl), 0) - tail
        return (rows.astype(F32) == labels).astype(F32).astype(BF16)

    def reduce(st, hot):
        rows = hm + EXTRA if st == 0 else hm
        put(u_out.at[st, 0, 1 - c], r_one.at[st, 0], sem_one, (st, 0), core)
        if st > 0:
            for p, to in ((0, to_x), (1, to_y)):
                put(u_out.at[st, 1 + p, c, :, pl.ds(0, width)], r_one.at[st, 1 + 2 * p, :, pl.ds(0, width)], sem_one, (st, 1 + 2 * p), {"days": to})
                put(u_out.at[st, 1 + p, 1 - c, :, pl.ds(0, width)], r_one.at[st, 2 + 2 * p, :, pl.ds(0, width)], sem_one, (st, 2 + 2 * p), {"days": to, "space": other})
        return rows

    def finish(st, hot, last):
        rows = hm + EXTRA if st == 0 else hm
        mine = u_out[st, 0, c]
        got(r_one.at[st, 0], sem_one, (st, 0), core)
        near = r_one[st, 0]
        value = mine[:, :width] + near[:, :width]
        if st > 0:
            gram = (mine[:, base:width] + near[:, base:width], mine[:, width:] + near[:, width:])
            parts = []
            for p, to in ((0, to_x), (1, to_y)):
                got(r_one.at[st, 1 + 2 * p, :, pl.ds(0, width)], sem_one, (st, 1 + 2 * p), {"days": to})
                got(r_one.at[st, 2 + 2 * p, :, pl.ds(0, width)], sem_one, (st, 2 + 2 * p), {"days": to, "space": other})
                far = r_one[st, 1 + 2 * p, :, :width] + r_one[st, 2 + 2 * p, :, :width]
                value = value + far
                parts.append(gram[p] + far[:, base:])
            low = jnp.where(lane < GRAM_AT, value[:, base:], parts[0] + parts[1])
            v_out[st, :, :base] = value[:, :base]
            v_out[st, :, base:] = low
        else:
            v_out[st] = value
        for k in range(1, nz):
            put(v_out.at[st], r_two.at[st, k - 1], sem_two, (st, k - 1), {"space": z_peer(k)})
        for k in range(1, nz):
            got(r_two.at[st, k - 1], sem_two, (st, k - 1), {"space": z_peer(k)})
        value = tree([v_out[st]] + [r_two[st, k - 1] for k in range(1, nz)])
        month = join3(nt(split3(value[:, :dl]), hot), hm)
        blk[st, 0, c, :hm, :base] = value[:, :base]
        blk[st, 0, c, :hm, base:] = value[:, base:] + month
        if st == 0:
            names = jnp.broadcast_to(l_ref[...].astype(F32), (EXTRA, dl))
            blk[st, 0, c, hm:, :base] = names[:, :base]
            blk[st, 0, c, hm:, base:] = nt(jnp.ones((EXTRA, dl), BF16), hot)
            blk[st, 0, c, hm:, base:dl] = names[:, base:]
        mine = blk.at[st, 0, c, pl.ds(0, rows)]
        put(mine, mine, sem_b, (st, 3), core)
        for p, to in ((0, to_x), (1, to_y), (2, to_d)):
            if p < 2 and not last:
                put(mine, blk.at[st, 1 + p, c, pl.ds(0, rows)], sem_b, (st, p), {"days": to})
            else:
                put(blk.at[st, 0, c, pl.ds(0, rows), pl.ds(base, LANES)], tl.at[st, p, c, pl.ds(0, rows)], sem_b, (st, p), {"days": to})
        theirs = blk.at[st, 0, 1 - c, pl.ds(0, rows)]
        got(theirs, sem_b, (st, 3), core)

    def landed(st, last, p, half):
        rows = hm + EXTRA if st == 0 else hm
        if p < 2 and not last:
            return blk.at[st, 1 + p, half, pl.ds(0, rows)]
        return tl.at[st, p, half, pl.ds(0, rows)]

    def forward(st, last):
        for p, to in ((0, to_x), (1, to_y), (2, to_d)):
            ref = landed(st, last, p, c)
            got(ref, sem_b, (st, p), {"days": to})
            put(ref, ref, sem_fw, (st, p), core)
        for p in range(3):
            got(landed(st, last, p, 1 - c), sem_fw, (st, p), core)

    def both(st, b):
        return jnp.concatenate([blk[st, b, 0, :hm], blk[st, b, 1, :hm]], axis=0)

    def tiles(st, last):
        out = [both(st, 0)[:, base:]]
        for p in range(3):
            if p < 2 and not last:
                out.append(both(st, 1 + p)[:, base:])
            else:
                out.append(jnp.concatenate([tl[st, p, 0, :hm], tl[st, p, 1, :hm]], axis=0))
        return out

    def mean_of(st, last, scale):
        sums = tree(tiles(st, last))
        inside = (lane >= tail) & (lane < tail + MONTHS)
        return split3(jnp.where(inside, sums * scale, 0.0))

    def center(value, mean, hot):
        return value - join3(nn(mean, hot), modes)

    own_hot = hot_of(l_ref[...].astype(F32))
    for half in range(2):
        u_out[0, 0, half] = jnp.zeros((hm, width + LANES), F32)
        u_out[0, 0, half, :, :dl] = total[half * hm : (half + 1) * hm]
    reduce(0, own_hot)
    finish(0, own_hot, False)
    for i in range(early, len(chunks)):
        send_fields(i)
    forward(0, False)
    hots = [own_hot] + [hot_of(blk[0, 1 + p, 0, hm : hm + 1, :dl]) for p in range(2)]
    counts = tree([blk[0, b, 0, hm : hm + 1, base:] for b in range(3)] + [tl[0, 2, 0, hm : hm + 1]])
    per_day = 1.0 / jnp.maximum(counts, 1.0)
    mean = mean_of(0, False, per_day)
    patterns = [split3(center(both(0, b)[:, :dl], mean, hots[b])) for b in range(3)]

    for it in range(ITERS):
        st = it + 1
        last = it == ITERS - 1
        for i, (at, w) in enumerate(chunks):
            for ab, to, back in ((0, to_x, to_y), (1, to_y, to_x)):
                if it == 0:
                    move(take, recv_f.at[ab, i], recv_f.at[ab, i], recv_t.at[ab], recv_t.at[ab], i, sem_f, (ab,), {"days": to})
                    part_f[ab, :, at : at + w] = value_of(recv_f.at[ab, i], recv_t.at[ab], i).astype(BF16)
                cover = join3(nn(patterns[0], own_f[row_of[ab], :, at : at + w])
                              + nn(patterns[1 + ab], part_f[ab, :, at : at + w]), modes)
                c_send[it, ab, i, :, :w] = cover
                if full[i] < w:
                    t_send[it, ab] = pack(cover[:, full[i] :], rest)
                move(put, c_send.at[it, ab, i], c_recv.at[it, ab, i], t_send.at[it, ab], t_recv.at[it, ab], i,
                     sem_c, (it, ab), {"days": back})
        raw = [None] * 3
        gram = [None] * 2

        def add(sums, k, term):
            sums[k] = term if sums[k] is None else sums[k] + term

        def spread(i):
            for ab, to in ((0, to_x), (1, to_y)):
                ref, ref_t = c_all.at[row_of[ab], i], t_all.at[row_of[ab]]
                move(put, ref, ref, ref_t, ref_t, i, sem_g, (ab,), {"days": to})

        for i, (at, w) in enumerate(chunks):
            for ab, back in ((0, to_y), (1, to_x)):
                move(take, c_recv.at[it, ab, i], c_recv.at[it, ab, i], t_recv.at[it, ab], t_recv.at[it, ab], i,
                     sem_c, (it, ab), {"days": back})
                scale = s_ref[row_of[ab]]
                cover = (c_send[it, ab, i, :, :w] + value_of(c_recv.at[it, ab, i], t_recv.at[it, ab], i)) * (scale * (1.0 / n_days))
                if last:
                    c_all[row_of[ab], i, :, :w] = cover
                    if full[i] < w:
                        t_all[row_of[ab]] = pack(cover[:, full[i] :], rest)
                padded = jnp.concatenate([jnp.zeros((GRAM_AT, w), F32), cover], axis=0)
                add(gram, ab, nt(cover, padded, precision=HIGH))
                cover3 = split3(cover * scale)
                add(raw, 0, nt(cover3, own_f[row_of[ab], :, at : at + w]))
                add(raw, 1 + ab, nt(cover3, part_f[ab, :, at : at + w]))
            if last and i == 0:
                spread(0)
        for b in range(3):
            whole = join3(raw[b], modes)
            for half in range(2):
                cut = slice(half * hm, (half + 1) * hm)
                u_out[st, b, half, :, base:width] = gram[max(b - 1, 0)][cut]
                if b == 0:
                    u_out[st, b, half, :, width:] = gram[1][cut]
                else:
                    u_out[st, b, half, :, width:] = jnp.zeros((hm, LANES), F32)
                u_out[st, b, half, :, :dl] = whole[cut]
        reduce(st, own_hot)
        if last:
            for i in range(1, len(chunks)):
                spread(i)
            for ab in range(2):
                pltpu.make_async_copy(c_all.at[row_of[ab]], cover_hbm.at[row_of[ab]], sem_o.at[ab]).start()
        finish(st, own_hot, last)
        inv = inverse_factor(both(st, 0)[:, base:])
        if not last:
            forward(st, last)
            mean = mean_of(st, last, per_day)
            patterns = [split3(nn(inv, center(both(st, b)[:, :dl], mean, hots[b]), precision=HIGH)) for b in range(3)]
        else:
            inv_ref[...] = inv
            for ab, to in ((0, to_x), (1, to_y)):
                row = row_out[ab]
                for i, (at, w) in enumerate(chunks):
                    move(take, c_all.at[row, i], c_all.at[row, i], t_all.at[row], t_all.at[row], i, sem_g, (ab,), {"days": to})
                if rest:
                    c_all[row, final, :, full[final] : chunks[final][1]] = unpack(t_all[row], rest)
                pltpu.make_async_copy(c_all.at[row], cover_hbm.at[row], sem_o.at[2 + ab]).start()
            forward(st, last)
            mean = mean_of(st, last, per_day)
            pcs_ref[...] = nn(inv, center(both(st, 0)[:, :dl], mean, own_hot), precision=HIGH)
    for k in range(2 * 2):
        row = (row_of + row_out)[k]
        pltpu.make_async_copy(c_all.at[row], cover_hbm.at[row], sem_o.at[k]).wait()
    for d in started:
        d.wait_send()


def solution(mesh):
    nd, ns = mesh.shape["days"], mesh.shape["space"]

    def local(fields, month_label, row_index, area_table, basis):
        dl, lat, lon = fields.shape
        modes = basis.shape[0]
        hm, nz = modes // 2, ns // 2
        base = dl // LANES * LANES
        width = base + LANES
        if nd != 4 or lat != nd or modes > GRAM_AT or dl - base + MONTHS > GRAM_AT or nz & (nz - 1):
            raise ValueError("unsupported sizes")
        n = -(-lon // CHUNK)
        stages = ITERS + 1
        v, dma = pltpu.VMEM, pltpu.SemaphoreType.DMA
        rest = lon % LANES
        if rest and (LANES % rest or modes * rest % (8 * LANES) or dl * rest % (8 * LANES)):
            raise ValueError("unsupported sizes")
        spare = max(rest, 8)
        cover, inv, pcs = pl.pallas_call(
            functools.partial(kernel, nd, ns),
            out_shape=(jax.ShapeDtypeStruct((lat, n, modes, CHUNK), F32), jax.ShapeDtypeStruct((modes, modes), F32),
                       jax.ShapeDtypeStruct((modes, dl), F32)),
            in_specs=[pl.BlockSpec(memory_space=pl.ANY)] * 2 + [pl.BlockSpec(memory_space=pltpu.SMEM)] * 2
            + [pl.BlockSpec(memory_space=v)],
            out_specs=(pl.BlockSpec(memory_space=pl.ANY),) + (pl.BlockSpec(memory_space=v),) * 2,
            scratch_shapes=[
                v((dl, lat, lon), BF16),
                v((modes, lat, lon), BF16),
                v((lat, dl, lon), BF16),
                v((2, n, dl, CHUNK), F32),
                v((2, n, dl, CHUNK), F32),
                v((2, dl * spare // LANES, LANES), F32),
                v((2, dl * spare // LANES, LANES), F32),
                v((2, dl, lon), BF16),
                v((lat, 1, 1), F32),
                v((stages, 3, 2, hm, width + LANES), F32),
                v((stages, 5, hm, width + LANES), F32),
                v((stages, hm, width), F32),
                v((stages, nz - 1, hm, width), F32),
                v((stages, 3, 2, hm + EXTRA, width), F32),
                v((stages, 3, 2, hm + EXTRA, LANES), F32),
                v((ITERS, 2, n, modes, CHUNK), F32),
                v((ITERS, 2, n, modes, CHUNK), F32),
                v((lat, n, modes, CHUNK), F32),
                v((ITERS, 2, modes * spare // LANES, LANES), F32),
                v((ITERS, 2, modes * spare // LANES, LANES), F32),
                v((lat, modes * spare // LANES, LANES), F32),
                dma((2,)), dma((2, 2, n + 1)), dma((2, stages, 5)), dma((2, stages, nz - 1)),
                dma((2, stages, 4)), dma((2, stages, 3)), dma((2, ITERS, 2, n + 1)), dma((2, 2, n + 1)),
                dma((4,)),
            ],
            compiler_params=pltpu.CompilerParams(
                collective_id=0, has_side_effects=True, vmem_limit_bytes=60 * 1024 * 1024),
        )(fields, basis, row_index, area_table, month_label[None, :])
        eofs, pcs = pl.pallas_call(
            last_kernel,
            grid=(n,),
            out_shape=(jax.ShapeDtypeStruct((modes, lat, lon), F32), jax.ShapeDtypeStruct((modes, dl), F32)),
            in_specs=[pl.BlockSpec((modes, modes), lambda i: (0, 0)),
                      pl.BlockSpec((lat, 1, modes, CHUNK), lambda i: (0, i, 0, 0)),
                      pl.BlockSpec((modes, dl), lambda i: (0, 0))],
            out_specs=(pl.BlockSpec((modes, lat, CHUNK), lambda i: (0, 0, i)), pl.BlockSpec((modes, dl), lambda i: (0, 0))),
        )(inv, cover, pcs)
        return eofs, pcs.T

    placed = (P("days", "space", None), P("days"), P("space"), P(), P(None, "space", None))
    return jax.shard_map(
        local,
        mesh=mesh,
        in_specs=placed,
        out_specs=(P(None, "space", None), P("days", None)),
        check_vma=False,
    )
```

```python
import functools

import jax
import jax.numpy as jnp
from jax import lax
from jax.experimental import pallas as pl
from jax.experimental.pallas import tpu as pltpu
from jax.sharding import PartitionSpec as P

ITERS = 2
MONTHS = 12
MESH = pl.DeviceIdType.MESH
F32 = jnp.float32
BF16 = jnp.bfloat16
LANES = 128
CHUNK = 3 * LANES
EXTRA = 8
GRAM_AT = LANES // 2
BLOCK = 4


def nt(a, b, **kw):
    return lax.dot_general(a, b, (((1,), (1,)), ((), ())), preferred_element_type=F32, **kw)


def nn(a, b, **kw):
    return lax.dot_general(a, b, (((1,), (0,)), ((), ())), preferred_element_type=F32, **kw)


def halves(x):
    high = x.astype(BF16)
    return high, (x - high.astype(F32)).astype(BF16)


def split(x):
    return jnp.concatenate(halves(x), axis=0)


def join(x):
    n = x.shape[0] // 2
    return x[:n] + x[n:]


def factor(inv):
    high, low = halves(inv)
    return jnp.concatenate([high, low, high, low], axis=1)


def apply(inv4, x):
    high, low = halves(x)
    return nn(inv4, jnp.concatenate([high, high, low, low], axis=0))


def tree(terms):
    while len(terms) > 1:
        terms = [terms[i] + terms[i + 1] for i in range(0, len(terms), 2)]
    return terms[0]


def pack(x, tail):
    rows = x.shape[0] * tail // LANES
    return jnp.concatenate([x[at : at + rows] for at in range(0, x.shape[0], rows)], axis=1)


def unpack(x, tail):
    return jnp.concatenate([x[:, at : at + tail] for at in range(0, LANES, tail)], axis=0)


def inverse_factor(tile):
    n = tile.shape[0]
    lane = lax.broadcasted_iota(jnp.int32, tile.shape, 1)
    sub = lax.broadcasted_iota(jnp.int32, tile.shape, 0)
    work = jnp.where(lane < GRAM_AT, (lane == sub).astype(F32), tile)
    for start in range(0, n, BLOCK):
        top = start // 8 * 8
        part = work[top:]
        rows = lax.broadcasted_iota(jnp.int32, part.shape, 0) + top
        at = GRAM_AT + start
        columns = [jnp.broadcast_to(part[:, at + t : at + t + 1], part.shape) for t in range(BLOCK)]
        for t in range(BLOCK):
            j = start + t
            k = j - top
            inv = lax.rsqrt(columns[t][k : k + 1])
            row = part[k : k + 1] * inv
            column = jnp.where(rows > j, columns[t] * inv, 0.0)
            for u in range(t + 1, BLOCK):
                columns[u] = columns[u] - column * column[k + u - t : k + u - t + 1]
            part = jnp.where(rows == j, row, part - column * row)
        work = part if top == 0 else jnp.concatenate([work[:top], part], axis=0)
    return work[:, :n]


def last_kernel(inv_ref, cover_ref, pcs_ref, eofs_ref, out_ref):
    inv4 = factor(inv_ref[...])
    for l in range(eofs_ref.shape[1]):
        eofs_ref[:, l, :] = apply(inv4, cover_ref[l, 0])
    out_ref[...] = pcs_ref[...]


def kernel(nd, ns, f_hbm, b_hbm, i_ref, a_ref, l_ref, cover_hbm, inv_hbm, pcs_hbm,
           inv_ref, pcs_ref, f_in, wide_f, b_in, own_f, send_f, recv_f, send_t, recv_t, part_f, s_ref,
           u_out, r_one, v_out, r_two, blk, tl, c_send, c_recv, c_all, t_send, t_recv, t_all,
           sem_l, sem_f, sem_one, sem_two, sem_b, sem_fw, sem_c, sem_g, sem_o):
    dl, lat, lon = f_in.shape
    modes = b_in.shape[0]
    hm = modes // 2
    base = dl // LANES * LANES
    tail = dl - base
    width = base + LANES
    nz = ns // 2
    chunks = [(at, min(CHUNK, lon - at)) for at in range(0, lon, CHUNK)]
    n_days = nd * dl
    rest = lon % LANES
    final = len(chunks) - 1
    full = [w // LANES * LANES for _, w in chunks]
    day, space = lax.axis_index("days"), lax.axis_index("space")
    x, y = lax.rem(day, 2), lax.div(day, 2)
    c, z = lax.rem(space, 2), lax.div(space, 2)
    to_x, to_y, to_d = day + 1 - 2 * x, day + 2 - 4 * y, nd - 1 - day
    other = space + 1 - 2 * c
    row_of = (x, lat // 2 + y)
    row_out = (1 - x, lat // 2 + 1 - y)

    def flip(v, k):
        for bit in range(k.bit_length()):
            if (k >> bit) & 1:
                v = v + (1 << bit) * (1 - 2 * lax.rem(lax.div(v, 1 << bit), 2))
        return v

    def z_peer(k):
        return flip(z, k) * 2 + c

    started = []

    def describe(src, dst, sems, index, device):
        return pltpu.make_async_remote_copy(
            src_ref=src, dst_ref=dst, send_sem=sems.at[(0,) + index], recv_sem=sems.at[(1,) + index],
            device_id=device, device_id_type=MESH)

    def put(src, dst, sems, index, device):
        d = describe(src, dst, sems, index, device)
        d.start()
        started.append(d)

    def got(dst, sems, index, device):
        describe(dst, dst, sems, index, device).wait_recv()

    core = {"space": other}
    barrier = pltpu.get_barrier_semaphore()
    friends = [core] + [{"space": z_peer(k)} for k in range(1, nz)]
    for d in (to_x, to_y, to_d):
        friends += [{"days": d}, {"days": d, "space": other}]
    for friend in friends:
        pl.semaphore_signal(barrier, inc=1, device_id=friend, device_id_type=MESH)
    load_f = pltpu.make_async_copy(f_hbm, f_in, sem_l.at[0])
    load_b = pltpu.make_async_copy(b_hbm, b_in, sem_l.at[1])
    load_f.start()
    load_b.start()
    for l in range(lat):
        s_ref[l] = jnp.sqrt(jnp.full((1, 1), a_ref[i_ref[l]], F32))
    load_f.wait()

    def move(act, src, dst, src_t, dst_t, i, sems, index, device):
        w = pl.ds(0, full[i])
        if full[i]:
            act(src.at[:, w], dst.at[:, w], sems, index + (i,), device)
        if i == final and rest:
            act(src_t, dst_t, sems, index + (i + 1,), device)

    def take(src, dst, sems, index, device):
        got(dst, sems, index, device)

    def value_of(ref, ref_t, i):
        main = ref[:, : full[i]]
        if i < final or not rest:
            return main
        return jnp.concatenate([main, unpack(ref_t[...], rest)], axis=1)

    def fill(ab, i):
        at, w = chunks[i]
        value = own_f[row_out[ab], :, at : at + w].astype(F32)
        send_f[ab, i, :, : full[i]] = value[:, : full[i]]
        if full[i] < w:
            send_t[ab] = pack(value[:, full[i] :], rest)

    def send_fields(i):
        for ab, to in ((0, to_x), (1, to_y)):
            move(put, send_f.at[ab, i], recv_f.at[ab, i], send_t.at[ab], recv_t.at[ab], i, sem_f, (ab,), {"days": to})

    early = len(chunks) - 1
    for i in range(len(chunks)):
        at, w = chunks[i]
        wide_f[i % 2, :, :, :w] = f_in[:, :, at : at + w].astype(F32)
        for l in range(lat):
            own_f[l, :, at : at + w] = wide_f[i % 2, :, l, :w].astype(BF16)
        for ab in range(2):
            fill(ab, i)
        if i == 0:
            pl.semaphore_wait(barrier, len(friends))
        if i < early:
            send_fields(i)

    load_b.wait()
    total = None
    for l in range(lat):
        term = nt(b_in[:, l, :], own_f[l]) * s_ref[l]
        total = term if total is None else total + term

    lane = lax.broadcasted_iota(jnp.int32, (1, LANES), 1)

    def hot_of(labels):
        rows = lax.broadcasted_iota(jnp.int32, (LANES, dl), 0) - tail
        return (rows.astype(F32) == labels).astype(F32).astype(BF16)

    def reduce(st, hot):
        rows = hm + EXTRA if st == 0 else hm
        put(u_out.at[st, 0, 1 - c], r_one.at[st, 0], sem_one, (st, 0), core)
        if st > 0:
            for p, to in ((0, to_x), (1, to_y)):
                put(u_out.at[st, 1 + p, c, :, pl.ds(0, width)], r_one.at[st, 1 + 2 * p, :, pl.ds(0, width)], sem_one, (st, 1 + 2 * p), {"days": to})
                put(u_out.at[st, 1 + p, 1 - c, :, pl.ds(0, width)], r_one.at[st, 2 + 2 * p, :, pl.ds(0, width)], sem_one, (st, 2 + 2 * p), {"days": to, "space": other})
        return rows

    def finish(st, hot, last):
        rows = hm + EXTRA if st == 0 else hm
        mine = u_out[st, 0, c]
        got(r_one.at[st, 0], sem_one, (st, 0), core)
        near = r_one[st, 0]
        value = mine[:, :width] + near[:, :width]
        if st > 0:
            gram = (mine[:, base:width] + near[:, base:width], mine[:, width:] + near[:, width:])
            parts = []
            for p, to in ((0, to_x), (1, to_y)):
                got(r_one.at[st, 1 + 2 * p, :, pl.ds(0, width)], sem_one, (st, 1 + 2 * p), {"days": to})
                got(r_one.at[st, 2 + 2 * p, :, pl.ds(0, width)], sem_one, (st, 2 + 2 * p), {"days": to, "space": other})
                far = r_one[st, 1 + 2 * p, :, :width] + r_one[st, 2 + 2 * p, :, :width]
                value = value + far
                parts.append(gram[p] + far[:, base:])
            low = jnp.where(lane < GRAM_AT, value[:, base:], parts[0] + parts[1])
            v_out[st, :, :base] = value[:, :base]
            v_out[st, :, base:] = low
        else:
            v_out[st] = value
        for k in range(1, nz):
            put(v_out.at[st], r_two.at[st, k - 1], sem_two, (st, k - 1), {"space": z_peer(k)})
        for k in range(1, nz):
            got(r_two.at[st, k - 1], sem_two, (st, k - 1), {"space": z_peer(k)})
        value = tree([v_out[st]] + [r_two[st, k - 1] for k in range(1, nz)])
        month = join(nt(split(value[:, :dl]), hot))
        blk[st, 0, c, :hm, :base] = value[:, :base]
        blk[st, 0, c, :hm, base:] = value[:, base:] + month
        if st == 0:
            names = jnp.broadcast_to(l_ref[...].astype(F32), (EXTRA, dl))
            blk[st, 0, c, hm:, :base] = names[:, :base]
            blk[st, 0, c, hm:, base:] = nt(jnp.ones((EXTRA, dl), BF16), hot)
            blk[st, 0, c, hm:, base:dl] = names[:, base:]
        mine = blk.at[st, 0, c, pl.ds(0, rows)]
        put(mine, mine, sem_b, (st, 3), core)
        for p, to in ((0, to_x), (1, to_y), (2, to_d)):
            if p < 2 and not last:
                put(mine, blk.at[st, 1 + p, c, pl.ds(0, rows)], sem_b, (st, p), {"days": to})
            else:
                tile = blk.at[st, 0, c, pl.ds(0, rows), pl.ds(base, LANES)]
                put(tile, tl.at[st, p, c, pl.ds(0, rows)], sem_b, (st, p), {"days": to})
                if last:
                    put(tile, tl.at[st, p, c, pl.ds(0, rows)], sem_fw, (st, p), {"days": to, "space": other})
        theirs = blk.at[st, 0, 1 - c, pl.ds(0, rows)]
        got(theirs, sem_b, (st, 3), core)

    def landed(st, last, p, half):
        rows = hm + EXTRA if st == 0 else hm
        if p < 2 and not last:
            return blk.at[st, 1 + p, half, pl.ds(0, rows)]
        return tl.at[st, p, half, pl.ds(0, rows)]

    def forward(st, last):
        for p, to in ((0, to_x), (1, to_y), (2, to_d)):
            ref = landed(st, last, p, c)
            got(ref, sem_b, (st, p), {"days": to})
            if not last:
                put(ref, ref, sem_fw, (st, p), core)
        for p, to in ((0, to_x), (1, to_y), (2, to_d)):
            device = {"days": to, "space": other} if last else core
            got(landed(st, last, p, 1 - c), sem_fw, (st, p), device)

    def both(st, b):
        return jnp.concatenate([blk[st, b, 0, :hm], blk[st, b, 1, :hm]], axis=0)

    def tiles(st, last):
        out = [both(st, 0)[:, base:]]
        for p in range(3):
            if p < 2 and not last:
                out.append(both(st, 1 + p)[:, base:])
            else:
                out.append(jnp.concatenate([tl[st, p, 0, :hm], tl[st, p, 1, :hm]], axis=0))
        return out

    def mean_of(st, last, scale):
        sums = tree(tiles(st, last))
        inside = (lane >= tail) & (lane < tail + MONTHS)
        return split(jnp.where(inside, sums * scale, 0.0))

    def center(value, mean, hot):
        return value - join(nn(mean, hot))

    own_hot = hot_of(l_ref[...].astype(F32))
    for half in range(2):
        u_out[0, 0, half] = jnp.zeros((hm, width + LANES), F32)
        u_out[0, 0, half, :, :dl] = total[half * hm : (half + 1) * hm]
    reduce(0, own_hot)
    finish(0, own_hot, False)
    for i in range(early, len(chunks)):
        send_fields(i)
    forward(0, False)
    hots = [own_hot] + [hot_of(blk[0, 1 + p, 0, hm : hm + 1, :dl]) for p in range(2)]
    counts = tree([blk[0, b, 0, hm : hm + 1, base:] for b in range(3)] + [tl[0, 2, 0, hm : hm + 1]])
    per_day = 1.0 / jnp.maximum(counts, 1.0)
    mean = mean_of(0, False, per_day)
    patterns = [split(center(both(0, b)[:, :dl], mean, hots[b])) for b in range(3)]

    for it in range(ITERS):
        st = it + 1
        last = it == ITERS - 1
        for i, (at, w) in enumerate(chunks):
            for ab, to, back in ((0, to_x, to_y), (1, to_y, to_x)):
                if it == 0:
                    move(take, recv_f.at[ab, i], recv_f.at[ab, i], recv_t.at[ab], recv_t.at[ab], i, sem_f, (ab,), {"days": to})
                    part_f[ab, :, at : at + w] = value_of(recv_f.at[ab, i], recv_t.at[ab], i).astype(BF16)
                cover = join(nn(patterns[0], own_f[row_of[ab], :, at : at + w])
                             + nn(patterns[1 + ab], part_f[ab, :, at : at + w]))
                c_send[it, ab, i, :, :w] = cover
                if full[i] < w:
                    t_send[it, ab] = pack(cover[:, full[i] :], rest)
                move(put, c_send.at[it, ab, i], c_recv.at[it, ab, i], t_send.at[it, ab], t_recv.at[it, ab], i,
                     sem_c, (it, ab), {"days": back})
        raw = [None] * 4
        gram = [None] * 2

        def add(sums, k, term):
            sums[k] = term if sums[k] is None else sums[k] + term

        def spread(i):
            for ab, to in ((0, to_x), (1, to_y)):
                ref, ref_t = c_all.at[row_of[ab], i], t_all.at[row_of[ab]]
                move(put, ref, ref, ref_t, ref_t, i, sem_g, (ab,), {"days": to})

        for i, (at, w) in enumerate(chunks):
            for ab, back in ((0, to_y), (1, to_x)):
                move(take, c_recv.at[it, ab, i], c_recv.at[it, ab, i], t_recv.at[it, ab], t_recv.at[it, ab], i,
                     sem_c, (it, ab), {"days": back})
                cover = (c_send[it, ab, i, :, :w] + value_of(c_recv.at[it, ab, i], t_recv.at[it, ab], i)) * (s_ref[row_of[ab]] * (1.0 / n_days))
                if last:
                    c_all[row_of[ab], i, :, :w] = cover
                    if full[i] < w:
                        t_all[row_of[ab]] = pack(cover[:, full[i] :], rest)
                cover2 = split(cover)
                add(gram, ab, nt(cover2, cover2))
                add(raw, 2 * ab, nt(cover2, own_f[row_of[ab], :, at : at + w]))
                add(raw, 2 * ab + 1, nt(cover2, part_f[ab, :, at : at + w]))
            if last and i == 0:
                spread(0)
        gram = [join(g) for g in gram]
        gram = [jnp.where(lane < GRAM_AT, 0.0, g + pltpu.roll(g, GRAM_AT, 1)) for g in gram]
        raw = [join(raw[k]) * s_ref[row_of[k // 2]] for k in range(4)]
        raw = (raw[0] + raw[2], raw[1], raw[3])
        for b in range(3):
            whole = raw[b]
            for half in range(2):
                cut = slice(half * hm, (half + 1) * hm)
                u_out[st, b, half, :, base:width] = gram[max(b - 1, 0)][cut]
                if b == 0:
                    u_out[st, b, half, :, width:] = gram[1][cut]
                else:
                    u_out[st, b, half, :, width:] = jnp.zeros((hm, LANES), F32)
                u_out[st, b, half, :, :dl] = whole[cut]
        reduce(st, own_hot)
        if last:
            for i in range(1, len(chunks)):
                spread(i)
            for ab in range(2):
                pltpu.make_async_copy(c_all.at[row_of[ab]], cover_hbm.at[row_of[ab]], sem_o.at[ab]).start()
        finish(st, own_hot, last)
        inv = inverse_factor(both(st, 0)[:, base:])
        inv4 = factor(inv)
        if not last:
            forward(st, last)
            mean = mean_of(st, last, per_day)
            patterns = [split(apply(inv4, center(both(st, b)[:, :dl], mean, hots[b]))) for b in range(3)]
        else:
            inv_ref[...] = inv
            pltpu.make_async_copy(inv_ref, inv_hbm, sem_o.at[4]).start()
            for ab, to in ((0, to_x), (1, to_y)):
                row = row_out[ab]
                for i, (at, w) in enumerate(chunks):
                    move(take, c_all.at[row, i], c_all.at[row, i], t_all.at[row], t_all.at[row], i, sem_g, (ab,), {"days": to})
                if rest:
                    c_all[row, final, :, full[final] : chunks[final][1]] = unpack(t_all[row], rest)
                pltpu.make_async_copy(c_all.at[row], cover_hbm.at[row], sem_o.at[2 + ab]).start()
            forward(st, last)
            mean = mean_of(st, last, per_day)
            pcs_ref[...] = apply(inv4, center(both(st, 0)[:, :dl], mean, own_hot))
            pltpu.make_async_copy(pcs_ref, pcs_hbm, sem_o.at[5]).start()
    for k in range(2 * 2):
        row = (row_of + row_out)[k]
        pltpu.make_async_copy(c_all.at[row], cover_hbm.at[row], sem_o.at[k]).wait()
    for d in started:
        d.wait_send()
    pltpu.make_async_copy(inv_ref, inv_hbm, sem_o.at[4]).wait()
    pltpu.make_async_copy(pcs_ref, pcs_hbm, sem_o.at[5]).wait()


def solution(mesh):
    nd, ns = mesh.shape["days"], mesh.shape["space"]

    def local(fields, month_label, row_index, area_table, basis):
        dl, lat, lon = fields.shape
        modes = basis.shape[0]
        hm, nz = modes // 2, ns // 2
        base = dl // LANES * LANES
        width = base + LANES
        if nd != 4 or lat != nd or modes != GRAM_AT or dl - base + MONTHS > GRAM_AT or nz & (nz - 1):
            raise ValueError("unsupported sizes")
        n = -(-lon // CHUNK)
        stages = ITERS + 1
        v, dma = pltpu.VMEM, pltpu.SemaphoreType.DMA
        rest = lon % LANES
        if rest and (LANES % rest or modes * rest % (8 * LANES) or dl * rest % (8 * LANES)):
            raise ValueError("unsupported sizes")
        spare = max(rest, 8)
        cover, inv, pcs = pl.pallas_call(
            functools.partial(kernel, nd, ns),
            out_shape=(jax.ShapeDtypeStruct((lat, n, modes, CHUNK), F32), jax.ShapeDtypeStruct((modes, modes), F32),
                       jax.ShapeDtypeStruct((modes, dl), F32)),
            in_specs=[pl.BlockSpec(memory_space=pl.ANY)] * 2 + [pl.BlockSpec(memory_space=pltpu.SMEM)] * 2
            + [pl.BlockSpec(memory_space=v)],
            out_specs=(pl.BlockSpec(memory_space=pl.ANY),) * 3,
            scratch_shapes=[
                v((modes, modes), F32),
                v((modes, dl), F32),
                v((dl, lat, lon), BF16),
                v((2, dl, lat, CHUNK), F32),
                v((modes, lat, lon), BF16),
                v((lat, dl, lon), BF16),
                v((2, n, dl, CHUNK), F32),
                v((2, n, dl, CHUNK), F32),
                v((2, dl * spare // LANES, LANES), F32),
                v((2, dl * spare // LANES, LANES), F32),
                v((2, dl, lon), BF16),
                v((lat, 1, 1), F32),
                v((stages, 3, 2, hm, width + LANES), F32),
                v((stages, 5, hm, width + LANES), F32),
                v((stages, hm, width), F32),
                v((stages, nz - 1, hm, width), F32),
                v((stages, 3, 2, hm + EXTRA, width), F32),
                v((stages, 3, 2, hm + EXTRA, LANES), F32),
                v((ITERS, 2, n, modes, CHUNK), F32),
                v((ITERS, 2, n, modes, CHUNK), F32),
                v((lat, n, modes, CHUNK), F32),
                v((ITERS, 2, modes * spare // LANES, LANES), F32),
                v((ITERS, 2, modes * spare // LANES, LANES), F32),
                v((lat, modes * spare // LANES, LANES), F32),
                dma((2,)), dma((2, 2, n + 1)), dma((2, stages, 5)), dma((2, stages, nz - 1)),
                dma((2, stages, 4)), dma((2, stages, 3)), dma((2, ITERS, 2, n + 1)), dma((2, 2, n + 1)),
                dma((6,)),
            ],
            compiler_params=pltpu.CompilerParams(
                collective_id=0, has_side_effects=True, vmem_limit_bytes=60 * 1024 * 1024),
        )(fields, basis, row_index, area_table, month_label[None, :])
        eofs, pcs = pl.pallas_call(
            last_kernel,
            grid=(n,),
            out_shape=(jax.ShapeDtypeStruct((modes, lat, lon), F32), jax.ShapeDtypeStruct((modes, dl), F32)),
            in_specs=[pl.BlockSpec((modes, modes), lambda i: (0, 0)),
                      pl.BlockSpec((lat, 1, modes, CHUNK), lambda i: (0, i, 0, 0)),
                      pl.BlockSpec((modes, dl), lambda i: (0, 0))],
            out_specs=(pl.BlockSpec((modes, lat, CHUNK), lambda i: (0, 0, i)), pl.BlockSpec((modes, dl), lambda i: (0, 0))),
        )(inv, cover, pcs)
        return eofs, pcs.T

    placed = (P("days", "space", None), P("days"), P("space"), P(), P(None, "space", None))
    return jax.shard_map(
        local,
        mesh=mesh,
        in_specs=placed,
        out_specs=(P(None, "space", None), P("days", None)),
        check_vma=False,
    )
```

```python
import functools

import jax
import jax.numpy as jnp
from jax import lax
from jax.experimental import pallas as pl
from jax.experimental.pallas import tpu as pltpu
from jax.sharding import PartitionSpec as P

ITERS = 2
MONTHS = 12
MESH = pl.DeviceIdType.MESH
F32 = jnp.float32
BF16 = jnp.bfloat16
LANES = 128
STEP = 4 * LANES
SIZES = (2, 3, 3, 2)
EARLY = 3
EXTRA = 8
GRAM_AT = LANES // 2
BLOCK = 4


def nt(a, b, **kw):
    return lax.dot_general(a, b, (((1,), (1,)), ((), ())), preferred_element_type=F32, **kw)


def nn(a, b, **kw):
    return lax.dot_general(a, b, (((1,), (0,)), ((), ())), preferred_element_type=F32, **kw)


def up(value, step):
    return -(-value // step) * step


def halves(x):
    high = x.astype(BF16)
    return high, (x - high.astype(F32)).astype(BF16)


def split(x):
    return jnp.concatenate(halves(x), axis=0)


def join(x):
    n = x.shape[0] // 2
    return x[:n] + x[n:]


def factor(inv):
    high, low = halves(inv)
    return jnp.concatenate([high, low, high, low], axis=1)


def apply(inv4, x):
    high, low = halves(x)
    return nn(inv4, jnp.concatenate([high, high, low, low], axis=0))


def cuts(lon):
    tiles = -(-lon // LANES)
    sizes = []
    for size in SIZES + (2,) * tiles:
        size = min(size, tiles - sum(sizes))
        if size:
            sizes.append(size)
    out, at = [], 0
    for size in sizes:
        out.append((at, min(size * LANES, lon - at)))
        at += size * LANES
    return out


def tree(terms):
    while len(terms) > 1:
        terms = [terms[i] + terms[i + 1] for i in range(0, len(terms), 2)]
    return terms[0]


def pack(x, tail):
    rows = x.shape[0] * tail // LANES
    return jnp.concatenate([x[at : at + rows] for at in range(0, x.shape[0], rows)], axis=1)


def unpack(x, tail):
    return jnp.concatenate([x[:, at : at + tail] for at in range(0, LANES, tail)], axis=0)


def inverse_factor(tile):
    n = tile.shape[0]
    lane = lax.broadcasted_iota(jnp.int32, tile.shape, 1)
    sub = lax.broadcasted_iota(jnp.int32, tile.shape, 0)
    work = jnp.where(lane < GRAM_AT, (lane == sub).astype(F32), tile)
    for start in range(0, n, BLOCK):
        top = start // 8 * 8
        part = work[top:]
        rows = lax.broadcasted_iota(jnp.int32, part.shape, 0) + top
        at = GRAM_AT + start
        columns = [jnp.broadcast_to(part[:, at + t : at + t + 1], part.shape) for t in range(BLOCK)]
        for t in range(BLOCK):
            j = start + t
            k = j - top
            inv = lax.rsqrt(columns[t][k : k + 1])
            row = part[k : k + 1] * inv
            column = jnp.where(rows > j, columns[t] * inv, 0.0)
            for u in range(t + 1, BLOCK):
                columns[u] = columns[u] - column * column[k + u - t : k + u - t + 1]
            part = jnp.where(rows == j, row, part - column * row)
        work = part if top == 0 else jnp.concatenate([work[:top], part], axis=0)
    return work[:, :n]


def last_kernel(inv_ref, cover_ref, pcs_ref, eofs_ref, out_ref):
    inv4 = factor(inv_ref[...])
    for l in range(eofs_ref.shape[1]):
        eofs_ref[:, l, :] = apply(inv4, cover_ref[l])
    out_ref[...] = pcs_ref[...]


def kernel(nd, ns, f_hbm, b_hbm, i_ref, a_ref, l_ref, cover_hbm, inv_hbm, pcs_hbm,
           inv_ref, pcs_ref, f_in, wide_f, b_in, own_f, send_f, recv_f, send_t, recv_t, part_f, s_ref,
           u_out, r_one, v_out, r_two, blk, tl, c_send, c_recv, c_all, t_send, t_recv, t_all,
           sem_l, sem_f, sem_one, sem_two, sem_b, sem_fw, sem_c, sem_g, sem_o):
    dl, lat, lon = f_in.shape
    modes = b_in.shape[0]
    hm = modes // 2
    base = dl // LANES * LANES
    tail = dl - base
    width = base + LANES
    nz = ns // 2
    chunks = cuts(lon)
    n_days = nd * dl
    rest = lon % LANES
    final = len(chunks) - 1
    full = [w // LANES * LANES for _, w in chunks]
    day, space = lax.axis_index("days"), lax.axis_index("space")
    x, y = lax.rem(day, 2), lax.div(day, 2)
    c, z = lax.rem(space, 2), lax.div(space, 2)
    to_x, to_y, to_d = day + 1 - 2 * x, day + 2 - 4 * y, nd - 1 - day
    other = space + 1 - 2 * c
    row_of = (x, lat // 2 + y)
    row_out = (1 - x, lat // 2 + 1 - y)

    def flip(v, k):
        for bit in range(k.bit_length()):
            if (k >> bit) & 1:
                v = v + (1 << bit) * (1 - 2 * lax.rem(lax.div(v, 1 << bit), 2))
        return v

    def z_peer(k):
        return flip(z, k) * 2 + c

    started = []

    def describe(src, dst, sems, index, device):
        return pltpu.make_async_remote_copy(
            src_ref=src, dst_ref=dst, send_sem=sems.at[(0,) + index], recv_sem=sems.at[(1,) + index],
            device_id=device, device_id_type=MESH)

    def put(src, dst, sems, index, device):
        d = describe(src, dst, sems, index, device)
        d.start()
        started.append(d)

    def got(dst, sems, index, device):
        describe(dst, dst, sems, index, device).wait_recv()

    core = {"space": other}
    barrier = pltpu.get_barrier_semaphore()
    friends = [core] + [{"space": z_peer(k)} for k in range(1, nz)]
    for d in (to_x, to_y, to_d):
        friends += [{"days": d}, {"days": d, "space": other}]
    for friend in friends:
        pl.semaphore_signal(barrier, inc=1, device_id=friend, device_id_type=MESH)
    load_f = pltpu.make_async_copy(f_hbm, f_in, sem_l.at[0])
    load_b = pltpu.make_async_copy(b_hbm, b_in, sem_l.at[1])
    load_f.start()
    load_b.start()
    for l in range(lat):
        s_ref[l] = jnp.sqrt(jnp.full((1, 1), a_ref[i_ref[l]], F32))
    load_f.wait()

    def move(act, src, dst, src_t, dst_t, i, sems, index, device):
        w = pl.ds(chunks[i][0], full[i])
        if full[i]:
            act(src.at[:, w], dst.at[:, w], sems, index + (i,), device)
        if i == final and rest:
            act(src_t, dst_t, sems, index + (i + 1,), device)

    def take(src, dst, sems, index, device):
        got(dst, sems, index, device)

    def value_of(ref, ref_t, i):
        main = ref[:, chunks[i][0] : chunks[i][0] + full[i]]
        if i < final or not rest:
            return main
        return jnp.concatenate([main, unpack(ref_t[...], rest)], axis=1)

    def send_fields(i):
        for ab, to in ((0, to_x), (1, to_y)):
            move(put, send_f.at[row_out[ab]], recv_f.at[ab], send_t.at[row_out[ab]], recv_t.at[ab], i, sem_f, (ab,), {"days": to})

    early = min(EARLY, len(chunks))
    for i in range(len(chunks)):
        at, w = chunks[i]
        wide_f[:, :, at : at + w] = f_in[:, :, at : at + w].astype(F32)
        for l in range(lat):
            value = wide_f[:, l, at : at + w]
            send_f[l, :, at : at + full[i]] = value[:, : full[i]]
            if full[i] < w:
                send_t[l] = pack(value[:, full[i] :], rest)
            own_f[l, :, at : at + w] = value.astype(BF16)
        if i == 0:
            pl.semaphore_wait(barrier, len(friends))
        if i < early:
            send_fields(i)
    load_b.wait()
    total = tree([nt(b_in[:, l, :], own_f[l]) * s_ref[l] for l in range(lat)])

    lane = lax.broadcasted_iota(jnp.int32, (1, LANES), 1)

    def hot_of(labels):
        rows = lax.broadcasted_iota(jnp.int32, (LANES, dl), 0) - tail
        return (rows.astype(F32) == labels).astype(F32).astype(BF16)

    def reduce(st, hot):
        rows = hm + EXTRA if st == 0 else hm
        put(u_out.at[st, 0, 1 - c], r_one.at[st, 0], sem_one, (st, 0), core)
        if st > 0:
            for p, to in ((0, to_x), (1, to_y)):
                put(u_out.at[st, 1 + p, c, :, pl.ds(0, width)], r_one.at[st, 1 + 2 * p, :, pl.ds(0, width)], sem_one, (st, 1 + 2 * p), {"days": to})
                put(u_out.at[st, 1 + p, 1 - c, :, pl.ds(0, width)], r_one.at[st, 2 + 2 * p, :, pl.ds(0, width)], sem_one, (st, 2 + 2 * p), {"days": to, "space": other})
        return rows

    def finish(st, hot, last):
        rows = hm + EXTRA if st == 0 else hm
        mine = u_out[st, 0, c]
        got(r_one.at[st, 0], sem_one, (st, 0), core)
        near = r_one[st, 0]
        value = mine[:, :width] + near[:, :width]
        if st > 0:
            gram = (mine[:, base:width] + near[:, base:width], mine[:, width:] + near[:, width:])
            parts = []
            for p, to in ((0, to_x), (1, to_y)):
                got(r_one.at[st, 1 + 2 * p, :, pl.ds(0, width)], sem_one, (st, 1 + 2 * p), {"days": to})
                got(r_one.at[st, 2 + 2 * p, :, pl.ds(0, width)], sem_one, (st, 2 + 2 * p), {"days": to, "space": other})
                far = r_one[st, 1 + 2 * p, :, :width] + r_one[st, 2 + 2 * p, :, :width]
                value = value + far
                parts.append(gram[p] + far[:, base:])
            low = jnp.where(lane < GRAM_AT, value[:, base:], parts[0] + parts[1])
            v_out[st, :, :base] = value[:, :base]
            v_out[st, :, base:] = low
        else:
            v_out[st] = value
        for k in range(1, nz):
            put(v_out.at[st], r_two.at[st, k - 1], sem_two, (st, k - 1), {"space": z_peer(k)})
        for k in range(1, nz):
            got(r_two.at[st, k - 1], sem_two, (st, k - 1), {"space": z_peer(k)})
        value = tree([v_out[st]] + [r_two[st, k - 1] for k in range(1, nz)])
        month = join(nt(split(value[:, :dl]), hot))
        blk[st, 0, c, :hm, :base] = value[:, :base]
        blk[st, 0, c, :hm, base:] = value[:, base:] + month
        if st == 0:
            names = jnp.broadcast_to(l_ref[...].astype(F32), (EXTRA, dl))
            blk[st, 0, c, hm:, :base] = names[:, :base]
            blk[st, 0, c, hm:, base:] = nt(jnp.ones((EXTRA, dl), BF16), hot)
            blk[st, 0, c, hm:, base:dl] = names[:, base:]
        mine = blk.at[st, 0, c, pl.ds(0, rows)]
        put(mine, mine, sem_b, (st, 3), core)
        for p, to in ((0, to_x), (1, to_y), (2, to_d)):
            if p < 2 and not last:
                put(mine, blk.at[st, 1 + p, c, pl.ds(0, rows)], sem_b, (st, p), {"days": to})
            else:
                tile = blk.at[st, 0, c, pl.ds(0, rows), pl.ds(base, LANES)]
                put(tile, tl.at[st, p, c, pl.ds(0, rows)], sem_b, (st, p), {"days": to})
                if last:
                    put(tile, tl.at[st, p, c, pl.ds(0, rows)], sem_fw, (st, p), {"days": to, "space": other})
        theirs = blk.at[st, 0, 1 - c, pl.ds(0, rows)]
        got(theirs, sem_b, (st, 3), core)

    def landed(st, last, p, half):
        rows = hm + EXTRA if st == 0 else hm
        if p < 2 and not last:
            return blk.at[st, 1 + p, half, pl.ds(0, rows)]
        return tl.at[st, p, half, pl.ds(0, rows)]

    def forward(st, last):
        for p, to in ((0, to_x), (1, to_y), (2, to_d)):
            ref = landed(st, last, p, c)
            got(ref, sem_b, (st, p), {"days": to})
            if not last:
                put(ref, ref, sem_fw, (st, p), core)
        for p, to in ((0, to_x), (1, to_y), (2, to_d)):
            device = {"days": to, "space": other} if last else core
            got(landed(st, last, p, 1 - c), sem_fw, (st, p), device)

    def both(st, b):
        return jnp.concatenate([blk[st, b, 0, :hm], blk[st, b, 1, :hm]], axis=0)

    def tiles(st, last):
        out = [both(st, 0)[:, base:]]
        for p in range(3):
            if p < 2 and not last:
                out.append(both(st, 1 + p)[:, base:])
            else:
                out.append(jnp.concatenate([tl[st, p, 0, :hm], tl[st, p, 1, :hm]], axis=0))
        return out

    def mean_of(st, last, scale):
        sums = tree(tiles(st, last))
        inside = (lane >= tail) & (lane < tail + MONTHS)
        return split(jnp.where(inside, sums * scale, 0.0))

    def center(value, mean, hot):
        return value - join(nn(mean, hot))

    own_hot = hot_of(l_ref[...].astype(F32))
    for half in range(2):
        u_out[0, 0, half] = jnp.zeros((hm, width + LANES), F32)
        u_out[0, 0, half, :, :dl] = total[half * hm : (half + 1) * hm]
    reduce(0, own_hot)
    finish(0, own_hot, False)
    for i in range(early, len(chunks)):
        send_fields(i)
    forward(0, False)
    hots = [own_hot] + [hot_of(blk[0, 1 + p, 0, hm : hm + 1, :dl]) for p in range(2)]
    counts = tree([blk[0, b, 0, hm : hm + 1, base:] for b in range(3)] + [tl[0, 2, 0, hm : hm + 1]])
    per_day = 1.0 / jnp.maximum(counts, 1.0)
    mean = mean_of(0, False, per_day)
    patterns = [split(center(both(0, b)[:, :dl], mean, hots[b])) for b in range(3)]

    for it in range(ITERS):
        st = it + 1
        last = it == ITERS - 1
        for i, (at, w) in enumerate(chunks):
            for ab, to, back in ((0, to_x, to_y), (1, to_y, to_x)):
                if it == 0:
                    move(take, recv_f.at[ab], recv_f.at[ab], recv_t.at[ab], recv_t.at[ab], i, sem_f, (ab,), {"days": to})
                    part_f[ab, :, at : at + w] = value_of(recv_f.at[ab], recv_t.at[ab], i).astype(BF16)
                cover = join(nn(patterns[0], own_f[row_of[ab], :, at : at + w])
                             + nn(patterns[1 + ab], part_f[ab, :, at : at + w]))
                c_send[it, ab, :, at : at + w] = cover
                if full[i] < w:
                    t_send[it, ab] = pack(cover[:, full[i] :], rest)
                move(put, c_send.at[it, ab], c_recv.at[it, ab], t_send.at[it, ab], t_recv.at[it, ab], i,
                     sem_c, (it, ab), {"days": back})
        raw = [None] * 4
        gram = [None] * 2

        def add(sums, k, term):
            sums[k] = term if sums[k] is None else sums[k] + term

        def spread(i):
            for ab, to in ((0, to_x), (1, to_y)):
                ref, ref_t = c_all.at[row_of[ab]], t_all.at[row_of[ab]]
                move(put, ref, ref, ref_t, ref_t, i, sem_g, (ab,), {"days": to})

        for i, (at, w) in enumerate(chunks):
            for ab, back in ((0, to_y), (1, to_x)):
                move(take, c_recv.at[it, ab], c_recv.at[it, ab], t_recv.at[it, ab], t_recv.at[it, ab], i,
                     sem_c, (it, ab), {"days": back})
                cover = (c_send[it, ab, :, at : at + w] + value_of(c_recv.at[it, ab], t_recv.at[it, ab], i)) * (s_ref[row_of[ab]] * (1.0 / n_days))
                if last:
                    c_all[row_of[ab], :, at : at + w] = cover
                    if full[i] < w:
                        t_all[row_of[ab]] = pack(cover[:, full[i] :], rest)
                cover2 = split(cover)
                add(gram, ab, nt(cover2, cover2))
                add(raw, 2 * ab, nt(cover2, own_f[row_of[ab], :, at : at + w]))
                add(raw, 2 * ab + 1, nt(cover2, part_f[ab, :, at : at + w]))
            if last and i == 0:
                spread(0)
        gram = [join(g) for g in gram]
        gram = [jnp.where(lane < GRAM_AT, 0.0, g + pltpu.roll(g, GRAM_AT, 1)) for g in gram]
        raw = [join(raw[k]) * s_ref[row_of[k // 2]] for k in range(4)]
        raw = (raw[0] + raw[2], raw[1], raw[3])
        for b in range(3):
            whole = raw[b]
            for half in range(2):
                cut = slice(half * hm, (half + 1) * hm)
                u_out[st, b, half, :, base:width] = gram[max(b - 1, 0)][cut]
                if b == 0:
                    u_out[st, b, half, :, width:] = gram[1][cut]
                else:
                    u_out[st, b, half, :, width:] = jnp.zeros((hm, LANES), F32)
                u_out[st, b, half, :, :dl] = whole[cut]
        reduce(st, own_hot)
        if last:
            for i in range(1, len(chunks)):
                spread(i)
            for ab in range(2):
                pltpu.make_async_copy(c_all.at[row_of[ab]], cover_hbm.at[row_of[ab]], sem_o.at[ab]).start()
        finish(st, own_hot, last)
        inv = inverse_factor(both(st, 0)[:, base:])
        inv4 = factor(inv)
        if not last:
            forward(st, last)
            mean = mean_of(st, last, per_day)
            patterns = [split(apply(inv4, center(both(st, b)[:, :dl], mean, hots[b]))) for b in range(3)]
        else:
            inv_ref[...] = inv
            pltpu.make_async_copy(inv_ref, inv_hbm, sem_o.at[4]).start()
            for ab, to in ((0, to_x), (1, to_y)):
                row = row_out[ab]
                for i, (at, w) in enumerate(chunks):
                    move(take, c_all.at[row], c_all.at[row], t_all.at[row], t_all.at[row], i, sem_g, (ab,), {"days": to})
                if rest:
                    c_all[row, :, lon - rest : lon] = unpack(t_all[row], rest)
                pltpu.make_async_copy(c_all.at[row], cover_hbm.at[row], sem_o.at[2 + ab]).start()
            forward(st, last)
            mean = mean_of(st, last, per_day)
            pcs_ref[...] = apply(inv4, center(both(st, 0)[:, :dl], mean, own_hot))
            pltpu.make_async_copy(pcs_ref, pcs_hbm, sem_o.at[5]).start()
    for k in range(2 * 2):
        row = (row_of + row_out)[k]
        pltpu.make_async_copy(c_all.at[row], cover_hbm.at[row], sem_o.at[k]).wait()
    for d in started:
        d.wait_send()
    pltpu.make_async_copy(inv_ref, inv_hbm, sem_o.at[4]).wait()
    pltpu.make_async_copy(pcs_ref, pcs_hbm, sem_o.at[5]).wait()


def solution(mesh):
    nd, ns = mesh.shape["days"], mesh.shape["space"]

    def local(fields, month_label, row_index, area_table, basis):
        dl, lat, lon = fields.shape
        modes = basis.shape[0]
        hm, nz = modes // 2, ns // 2
        base = dl // LANES * LANES
        width = base + LANES
        if nd != 4 or lat != nd or modes != GRAM_AT or dl - base + MONTHS > GRAM_AT or nz & (nz - 1):
            raise ValueError("unsupported sizes")
        n, span = len(cuts(lon)), up(lon, LANES)
        stages = ITERS + 1
        v, dma = pltpu.VMEM, pltpu.SemaphoreType.DMA
        rest = lon % LANES
        if rest and (LANES % rest or modes * rest % (8 * LANES) or dl * rest % (8 * LANES)):
            raise ValueError("unsupported sizes")
        spare = max(rest, 8)
        cover, inv, pcs = pl.pallas_call(
            functools.partial(kernel, nd, ns),
            out_shape=(jax.ShapeDtypeStruct((lat, modes, span), F32), jax.ShapeDtypeStruct((modes, modes), F32),
                       jax.ShapeDtypeStruct((modes, dl), F32)),
            in_specs=[pl.BlockSpec(memory_space=pl.ANY)] * 2 + [pl.BlockSpec(memory_space=pltpu.SMEM)] * 2
            + [pl.BlockSpec(memory_space=v)],
            out_specs=(pl.BlockSpec(memory_space=pl.ANY),) * 3,
            scratch_shapes=[
                v((modes, modes), F32),
                v((modes, dl), F32),
                v((dl, lat, lon), BF16),
                v((dl, lat, span), F32),
                v((modes, lat, lon), BF16),
                v((lat, dl, lon), BF16),
                v((lat, dl, span), F32),
                v((2, dl, span), F32),
                v((lat, dl * spare // LANES, LANES), F32),
                v((2, dl * spare // LANES, LANES), F32),
                v((2, dl, lon), BF16),
                v((lat, 1, 1), F32),
                v((stages, 3, 2, hm, width + LANES), F32),
                v((stages, 5, hm, width + LANES), F32),
                v((stages, hm, width), F32),
                v((stages, nz - 1, hm, width), F32),
                v((stages, 3, 2, hm + EXTRA, width), F32),
                v((stages, 3, 2, hm + EXTRA, LANES), F32),
                v((ITERS, 2, modes, span), F32),
                v((ITERS, 2, modes, span), F32),
                v((lat, modes, span), F32),
                v((ITERS, 2, modes * spare // LANES, LANES), F32),
                v((ITERS, 2, modes * spare // LANES, LANES), F32),
                v((lat, modes * spare // LANES, LANES), F32),
                dma((2,)), dma((2, 2, n + 1)), dma((2, stages, 5)), dma((2, stages, nz - 1)),
                dma((2, stages, 4)), dma((2, stages, 3)), dma((2, ITERS, 2, n + 1)), dma((2, 2, n + 1)),
                dma((6,)),
            ],
            compiler_params=pltpu.CompilerParams(
                collective_id=0, has_side_effects=True, vmem_limit_bytes=60 * 1024 * 1024),
        )(fields, basis, row_index, area_table, month_label[None, :])
        eofs, pcs = pl.pallas_call(
            last_kernel,
            grid=(-(-span // STEP),),
            out_shape=(jax.ShapeDtypeStruct((modes, lat, lon), F32), jax.ShapeDtypeStruct((modes, dl), F32)),
            in_specs=[pl.BlockSpec((modes, modes), lambda i: (0, 0)),
                      pl.BlockSpec((lat, modes, STEP), lambda i: (0, 0, i)),
                      pl.BlockSpec((modes, dl), lambda i: (0, 0))],
            out_specs=(pl.BlockSpec((modes, lat, STEP), lambda i: (0, 0, i)), pl.BlockSpec((modes, dl), lambda i: (0, 0))),
        )(inv, cover, pcs)
        return eofs, pcs.T

    placed = (P("days", "space", None), P("days"), P("space"), P(), P(None, "space", None))
    return jax.shard_map(
        local,
        mesh=mesh,
        in_specs=placed,
        out_specs=(P(None, "space", None), P("days", None)),
        check_vma=False,
    )
```
